32 devices in a mesh: pair: 4 (over y, x), aux: 8 (over z, core).
Axes of the slice: x: 2, y: 2, z: 4, core: 2. Of those that a mesh axis runs over, the one named last changes fastest.
Arguments:
- amplitudes: bfloat16 [4, 512, 512], P('pair', 'aux'), may hold values from -6 to 6
- factors: bfloat16 [4096, 512, 512], P('aux', 'pair'), may hold values from -0.03125 to 0.03125
- hole_weights: float32 [4, 4], replicated, may hold values from -3 to 3
- driver: float32 [4, 6, 512], P('pair', None, 'aux'), may hold values from -6 to 6
- eps_vir: float32 [512], replicated, may hold values from 0.5 to 3
- pair_energy: float32 [4], P('pair'), may hold values from -3 to -0.5
Outputs:
- residual: float32 [4, 6, 512], P('pair', None, 'aux')
- new_amps: float32 [4, 6, 512], P('pair', None, 'aux')
The draws below stay inside these ranges and needn't reach their ends.
All inputs are finite; a program needn't handle non-finite values.
Results may differ from the reference program's by a relative error of at most 0.0003.
Values may be sent and summed in bfloat16 or wider, within the bound.
A program may use at most 192 MiB of HBM per device.

```python
import jax
import jax.numpy as jnp
from jax import lax

V = 512
NAUX = 4096
A = 6
P_SIZE = 4


def block_levels(key, extent, pieces, least, largest):
    level, own = 1.0, jax.random.fold_in(key, 6)
    for axis_at, parts in pieces:
        draws = jnp.exp(jax.random.uniform(jax.random.fold_in(own, axis_at), (parts,), jnp.float32, least / len(pieces), largest / len(pieces)))
        level = level * jnp.repeat(draws, extent[axis_at] // parts).reshape([-1 if axis == axis_at else 1 for axis in range(len(extent))])
    return level


def scatter_about(own_key, dims, width, reach, cuts=(), dtype=jnp.bfloat16):
    gain = block_levels(own_key, dims, cuts, -0.22, 0.18) if cuts else 1.0
    entries = jax.random.normal(own_key, dims, jnp.float32) * width * gain
    return jnp.minimum(jnp.maximum(entries, -reach), reach).astype(dtype)


def setup_inputs(seed: int = 0) -> dict:
    key_of = jax.random.split(jax.random.key(seed), 7)
    return {
        "amplitudes": scatter_about(key_of[0], (P_SIZE, V, V), 1.0, 6.0, ((0, 4), (1, 8))),
        "factors": scatter_about(key_of[1], (NAUX, V, V), (V * 64) ** -0.5, 0.03125, ((0, 8), (1, 4))),
        "hole_weights": scatter_about(key_of[2], (P_SIZE, P_SIZE), P_SIZE ** -0.5, 3.0, (), jnp.float32),
        "driver": scatter_about(key_of[3], (P_SIZE, A, V), 1.0, 6.0, ((0, 4), (2, 8)), jnp.float32),
        "eps_vir": jnp.clip(jax.random.uniform(key_of[4], (V,), jnp.float32, 0.5, 3.0), 0.5, 3.0),
        "pair_energy": jnp.clip(-3.0 + 2.5 * jax.random.uniform(key_of[5], (P_SIZE,), jnp.float32) ** block_levels(key_of[5], (P_SIZE,), ((0, 4),), -0.2, 0.2), -3.0, -0.5),
    }


def reference(amplitudes, factors, hole_weights, driver, eps_vir, pair_energy):
    block_size = min(128, NAUX)
    block_count = NAUX // block_size
    amp_wide = amplitudes.astype(jnp.float32)
    stacked = factors.reshape(block_count, block_size, V, V)

    def add_block(total, factor_block):
        wide = factor_block.astype(jnp.float32)
        halves = jnp.einsum("qac,pcd->paqd", wide[:, :A, :], amp_wide, precision=lax.Precision.HIGHEST).astype(jnp.bfloat16)
        term = jnp.einsum("paqd,qbd->pab", halves.astype(jnp.float32), wide, precision=lax.Precision.HIGHEST)
        return total + term, None

    particle, unused = lax.scan(add_block, jnp.zeros((P_SIZE, A, V), jnp.float32), stacked)
    amp_window = amp_wide[:, :A, :]
    hole_term = jnp.einsum("pk,kab->pab", hole_weights, amp_window, precision=lax.Precision.HIGHEST)
    residual = driver + particle + hole_term
    denominator = eps_vir[:A][None, :, None] + eps_vir[None, None, :] - pair_energy[:, None, None]
    new_amps = amp_window - residual / denominator
    return residual, new_amps
```

```python
import functools

import jax
import jax.numpy as jnp
from jax import lax
from jax.experimental import pallas as pl
from jax.experimental.pallas import tpu as pltpu
from jax.sharding import PartitionSpec as P

MESH = pl.DeviceIdType.MESH
F32 = jnp.float32
BF16 = jnp.bfloat16


def ring_order(n):
    side = 1
    while side * side < n:
        side += 1
    if side * side != n or side % 2:
        return list(range(n))
    order = []
    for row in range(side):
        cols = list(range(1, side))
        if row % 2:
            cols.reverse()
        if row == 0:
            cols = [0] + cols
        order += [row * side + col for col in cols]
    order += [row * side for row in range(side - 1, 0, -1)]
    return order


def lookup(index, table):
    value = jnp.int32(table[0])
    for at, entry in enumerate(table[1:], 1):
        value = jnp.where(index == at, jnp.int32(entry), value)
    return value


def kernel(
    n_pair, n_aux, rows, chunk, slots,
    amp_ref, win_ref, fac_ref,
    sum_ref, slab_ref,
    t_ref, w_ref, f_ref, h_ref, e_ref, part_ref, got_ref,
    f_sem, loc_sem, wl_sem, a_send, a_recv, z_send, z_recv, c_send, c_recv, w_send, w_recv, r_send, r_recv,
):
    width = amp_ref.shape[2]
    own_rows = amp_ref.shape[1]
    block = fac_ref.shape[1]
    chunks = w_ref.shape[0]
    pad = 8
    m = n_aux // 2
    i = lax.axis_index("pair")
    j = lax.axis_index("aux")
    z = j // 2
    core = lax.rem(j, 2)

    order = ring_order(n_pair)
    where = [order.index(k) for k in range(n_pair)]
    pos = lookup(i, where)
    right = lookup(i, [order[(where[k] + 1) % n_pair] for k in range(n_pair)])
    left = lookup(i, [order[(where[k] - 1) % n_pair] for k in range(n_pair)])

    def rows_of(at):
        return pl.ds(pl.multiple_of(at * own_rows, own_rows), own_rows)

    def load_factors(k):
        slot = lax.rem(k, slots)
        return pltpu.make_async_copy(
            fac_ref.at[pl.ds(pl.multiple_of(k * chunk, chunk), chunk)], f_ref.at[slot], f_sem.at[slot]
        )

    local = pltpu.make_async_copy(amp_ref.at[0], t_ref.at[i, rows_of(j)], loc_sem)
    local.start()

    def a_copy(peer, source):
        return pltpu.make_async_remote_copy(
            src_ref=amp_ref.at[0], dst_ref=t_ref.at[source, rows_of(j)],
            send_sem=a_send.at[peer], recv_sem=a_recv.at[source],
            device_id=(peer, j), device_id_type=MESH,
        )

    for step in range(1, n_pair):
        peer = lax.rem(i + step, n_pair)
        a_copy(peer, i).start()

    def w_load(k):
        return pltpu.make_async_copy(win_ref.at[k], w_ref.at[k], wl_sem.at[k])

    def w_copy(k, target):
        return pltpu.make_async_remote_copy(
            src_ref=w_ref.at[k], dst_ref=w_ref.at[k],
            send_sem=w_send.at[k], recv_sem=w_recv.at[k],
            device_id=(target, j), device_id_type=MESH,
        )

    def target_of(k):
        return jnp.where(lax.rem(k, 2) == 0, right, left)

    def distance(k):
        return jnp.where(lax.rem(k, 2) == 0, pos, lax.rem(n_pair - pos, n_pair))

    @pl.when(pos == 0)
    def _():
        @pl.loop(0, chunks)
        def _(k):
            w_load(k).start()

        @pl.loop(0, chunks)
        def _(k):
            w_load(k).wait()
            w_copy(k, target_of(k)).start()

    for k in range(slots):
        load_factors(k).start()

    e_row = lax.broadcasted_iota(jnp.int32, e_ref.shape, 0)
    e_col = lax.broadcasted_iota(jnp.int32, e_ref.shape, 1)
    hit = (e_col == (e_row // pad) * rows + e_row % pad) & (e_row % pad < rows)
    e_ref[...] = jnp.where(hit, 1.0, 0.0).astype(BF16)

    local.wait()
    for step in range(1, n_pair):
        source = lax.rem(i + n_pair - step, n_pair)
        a_copy(i, source).wait_recv()

    def z_copy(peer, source):
        return pltpu.make_async_remote_copy(
            src_ref=t_ref.at[:, rows_of(j)], dst_ref=t_ref.at[:, rows_of(source * 2 + core)],
            send_sem=z_send.at[peer], recv_sem=z_recv.at[source],
            device_id=(i, peer * 2 + core), device_id_type=MESH,
        )

    def c_copy(source, own):
        held = rows_of(source * 2 + own)
        return pltpu.make_async_remote_copy(
            src_ref=t_ref.at[:, held], dst_ref=t_ref.at[:, held],
            send_sem=c_send.at[source], recv_sem=c_recv.at[source],
            device_id=(i, z * 2 + 1 - core), device_id_type=MESH,
        )

    for step in range(1, m):
        z_copy(lax.rem(z + step, m), z).start()
    c_copy(z, core).start()
    for step in range(1, m):
        source = lax.rem(z + m - step, m)
        z_copy(z, source).wait_recv()
        c_copy(source, core).start()

    def handle(k):
        dist = distance(k)
        w_copy(k, target_of(k)).wait_recv()

        @pl.when(dist < n_pair - 1)
        def _():
            w_copy(k, target_of(k)).start()

    def look(k):
        return 2 * (n_pair - 1 - distance(k))

    @pl.when(pos > 0)
    def _():
        @pl.loop(0, chunks)
        def _(k):
            @pl.when(k < look(k))
            def _():
                handle(k)

    for source in range(m):
        c_copy(source, 1 - core).wait_recv()

    part_ref[...] = jnp.zeros_like(part_ref)

    @pl.loop(0, chunks)
    def _(k):
        ahead = k + look(k)

        @pl.when((pos > 0) & (ahead < chunks))
        def _():
            handle(ahead)

        wide = jnp.dot(e_ref[...], w_ref[k], preferred_element_type=F32).astype(BF16)
        for p in range(0, n_pair, 2):
            two = [
                jnp.dot(wide, t_ref[p + at], preferred_element_type=F32).reshape(chunk, pad, width)
                for at in range(2)
            ]
            h_ref[:, p * pad : (p + 2) * pad, :] = jnp.concatenate(two, axis=1).astype(BF16)
        load_factors(k).wait()
        slot = lax.rem(k, slots)

        def add(q, total):
            return total + lax.dot_general(
                f_ref[slot, q], h_ref[q], (((1,), (1,)), ((), ())), preferred_element_type=F32
            )

        total = lax.fori_loop(0, chunk, add, jnp.zeros((block, n_pair * pad), F32), unroll=8)
        part_ref[...] += total.T.reshape(n_pair, pad, block)

        @pl.when(k + slots < chunks)
        def _():
            load_factors(k + slots).start()

    ratio = n_aux // n_pair

    def r_copy(p, t, source, to):
        return pltpu.make_async_remote_copy(
            src_ref=part_ref.at[p], dst_ref=got_ref.at[source],
            send_sem=r_send.at[p * ratio + t], recv_sem=r_recv.at[source],
            device_id=to, device_id_type=MESH,
        )

    for p in range(n_pair):
        for t in range(ratio):
            column = i * ratio + t
            mine = (i == p) & (j == column)

            @pl.when(mine)
            def _():
                got_ref[j] = part_ref[p]

            @pl.when(jnp.logical_not(mine))
            def _():
                r_copy(p, t, j, (jnp.int32(p), column)).start()

    slab_ref[...] = t_ref[:, 0:16, :]
    column_owner = j // ratio
    for source in range(n_aux):
        @pl.when(jnp.logical_not((column_owner == i) & (j == source)))
        def _():
            r_copy(0, 0, source, (i, j)).wait_recv()

    total = got_ref[0]
    for source in range(1, n_aux):
        total = total + got_ref[source]
    sum_ref[...] = total

    for p in range(n_pair):
        for t in range(ratio):
            column = i * ratio + t

            @pl.when(jnp.logical_not((i == p) & (j == column)))
            def _():
                r_copy(p, t, j, (jnp.int32(p), column)).wait_send()
    for step in range(1, n_pair):
        a_copy(lax.rem(i + step, n_pair), i).wait_send()
    for step in range(1, m):
        z_copy(lax.rem(z + step, m), z).wait_send()
    for source in range(m):
        c_copy(source, core).wait_send()

    @pl.loop(0, chunks)
    def _(k):
        @pl.when(distance(k) < n_pair - 1)
        def _():
            w_copy(k, target_of(k)).wait_send()


def per_device(n_pair, n_aux, amplitudes, factors, hole_weights, driver, eps_vir, pair_energy):
    rows, columns = driver.shape[1:]
    depth, block, width = factors.shape
    own_rows = amplitudes.shape[1]
    chunk = min(32, depth)
    chunks = depth // chunk
    slots = min(8, chunks)
    window = factors[:, :rows, :].reshape(chunks, chunk * rows, width)
    pad = 8
    m = n_aux // 2
    ratio = n_aux // n_pair
    vmem = pl.BlockSpec(memory_space=pltpu.VMEM)
    hbm = pl.BlockSpec(memory_space=pl.ANY)
    dma = pltpu.SemaphoreType.DMA
    summed, slab = pl.pallas_call(
        functools.partial(kernel, n_pair, n_aux, rows, chunk, slots),
        out_shape=(
            jax.ShapeDtypeStruct((pad, block), F32),
            jax.ShapeDtypeStruct((n_pair, 16, width), BF16),
        ),
        in_specs=[hbm, hbm, hbm],
        out_specs=(vmem, vmem),
        scratch_shapes=[
            pltpu.VMEM((n_pair, n_aux * own_rows, width), BF16),
            pltpu.VMEM((chunks, chunk * rows, width), BF16),
            pltpu.VMEM((slots, chunk, block, width), BF16),
            pltpu.VMEM((chunk, n_pair * pad, width), BF16),
            pltpu.VMEM((chunk * pad, chunk * rows), BF16),
            pltpu.VMEM((n_pair, pad, block), F32),
            pltpu.VMEM((n_aux, pad, block), F32),
            dma((slots,)),
            dma,
            dma((chunks,)),
            dma((n_pair,)),
            dma((n_pair,)),
            dma((m,)),
            dma((m,)),
            dma((m,)),
            dma((m,)),
            dma((chunks,)),
            dma((chunks,)),
            dma((n_pair * ratio,)),
            dma((n_aux,)),
        ],
        compiler_params=pltpu.CompilerParams(has_side_effects=True, vmem_limit_bytes=60 * 1024 * 1024),
    )(amplitudes, window, factors)

    pair_index = lax.axis_index("pair")
    aux_index = lax.axis_index("aux")
    start = aux_index * columns
    slab_cols = lax.dynamic_slice_in_dim(slab[:, :rows], start, columns, 2).astype(F32)
    weights = lax.dynamic_slice_in_dim(hole_weights, pair_index, 1, 0)[0]
    hole = weights[0] * slab_cols[0]
    for k in range(1, n_pair):
        hole = hole + weights[k] * slab_cols[k]
    particle = lax.dynamic_slice_in_dim(summed[:rows], lax.rem(aux_index, ratio) * columns, columns, 1)
    residual = driver + (particle + hole)[None]
    amp_cols = lax.dynamic_slice_in_dim(slab_cols, pair_index, 1, 0)
    eps_cols = lax.dynamic_slice_in_dim(eps_vir, start, columns, 0)
    denominator = eps_vir[:rows][None, :, None] + eps_cols[None, None, :] - pair_energy[:, None, None]
    return residual, amp_cols - residual / denominator


def solution(mesh):
    return jax.shard_map(
        functools.partial(per_device, mesh.shape["pair"], mesh.shape["aux"]),
        mesh=mesh,
        in_specs=(
            P("pair", "aux", None),
            P("aux", "pair", None),
            P(),
            P("pair", None, "aux"),
            P(),
            P("pair"),
        ),
        out_specs=(P("pair", None, "aux"), P("pair", None, "aux")),
        check_vma=False,
    )
```
